32 devices in a mesh: section: 2 (over x), expert: 16 (over z, y, core).
Axes of the slice: x: 2, y: 2, z: 4, core: 2. Of those that a mesh axis runs over, the one named last changes fastest.
Arguments:
- images: bfloat16 [32, 256, 1408], P(('section', 'expert')), may hold values from -6 to 6
- norm_gain: bfloat16 [1408], replicated, may hold values from 0.5 to 1.5
- slot_map: bfloat16 [1408, 16], replicated, may hold values from -0.15625 to 0.15625
- logit_scale: float32 [1], replicated, may hold values from 30 to 80
- up_weight: bfloat16 [16, 5120, 1408], P('expert', 'section'), may hold values from -0.625 to 0.625
- down_weight: bfloat16 [16, 5120, 1408], P('expert', 'section'), may hold values from -0.3125 to 0.3125
Outputs:
- block_out: bfloat16 [32, 256, 1408], P(('section', 'expert'))
The draws below stay inside these ranges and needn't reach their ends.
All inputs are finite; a program needn't handle non-finite values.
Results may differ from the reference program's by a relative error of at most 0.011.
Values may be sent and summed in bfloat16 or wider, within the bound.
No kernel may reach another device: no remote copies, remote signals or barrier semaphores. Data moves between devices by JAX's collectives and lax.ppermute only.
A program may use at most 64 MiB of HBM per device.

```python
import math
import jax
import jax.numpy as jnp
from jax import lax

D = 1408
FF = 5120
TOK = 256
EXPERTS = 16
IMAGES = 32


def levels(rng, extent, shards, low, top_value):
    def one(axis_at, shards_of):
        heights = jax.random.uniform(jax.random.fold_in(jax.random.fold_in(rng, 6), axis_at), (shards_of,), jnp.float32, low / len(shards), top_value / len(shards))
        return jnp.repeat(jnp.exp(heights), extent[axis_at] // shards_of).reshape((-1,) + (1,) * (len(extent) - axis_at - 1))

    loudness = one(*shards[0])
    for cut in shards[1:]:
        loudness = loudness * one(*cut)
    return loudness


def centred(own_key, extent, deviation, reach, split=(), kind=jnp.bfloat16):
    level = levels(own_key, extent, split, -0.22, 0.18) if split else 1.0
    result = jax.random.normal(own_key, extent, jnp.float32) * deviation * level
    return jnp.minimum(jnp.maximum(result, -reach), reach).astype(kind)


def setup_inputs(seed: int = 0) -> dict:
    key_list = jax.random.split(jax.random.key(seed), 7)
    images = centred(key_list[0], (IMAGES, TOK, D), 1.0, 6.0, ((0, 32),))
    norm_gain = jnp.clip(1.0 + 0.1 * jax.random.normal(key_list[1], (D,), jnp.float32), 0.5, 1.5).astype(jnp.bfloat16)
    slot_map = centred(key_list[2], (D, EXPERTS), D ** -0.5, 0.15625)
    logit_scale = jnp.clip(jnp.exp(jax.random.uniform(key_list[3], (1,), jnp.float32, math.log(30.0), math.log(80.0))), 30.0, 80.0)
    up_weight = centred(key_list[4], (EXPERTS, FF, D), (4.0 / D ** 0.5), 0.625, ((0, 16), (1, 2)))
    down_weight = centred(key_list[5], (EXPERTS, FF, D), (4.0 / FF ** 0.5), 0.3125, ((0, 16), (1, 2)))
    return dict(images=images, norm_gain=norm_gain, slot_map=slot_map, logit_scale=logit_scale, up_weight=up_weight, down_weight=down_weight)


epsilon = 1e-06

def normalize(inputs, gain_row):
    values = inputs.astype(jnp.float32)
    spread = lax.optimization_barrier(jnp.mean(values * values, axis=-1, keepdims=True))
    return (values * lax.rsqrt(spread + epsilon) * gain_row.astype(jnp.float32)).astype(jnp.bfloat16)

def weights_from(raw, normed, slot_cols, scale_now):
    values = normed.astype(jnp.float32)
    token_norm = jnp.sqrt(lax.optimization_barrier(jnp.sum(values * values, axis=-1)) + epsilon)
    columns = slot_cols.astype(jnp.float32)
    column_norm = jnp.sqrt(lax.optimization_barrier(jnp.sum(columns * columns, axis=0)) + epsilon)
    logits = scale_now * raw / (token_norm[:, None, :] * column_norm[None, :, None])
    scores = jnp.exp(logits)
    dispatch = (scores / lax.optimization_barrier(jnp.sum(scores, axis=-1, keepdims=True))).astype(jnp.bfloat16)
    combine = (scores / lax.optimization_barrier(jnp.sum(scores, axis=1, keepdims=True))).astype(jnp.bfloat16)
    return (dispatch, combine)

def reference(images, norm_gain, slot_map, logit_scale, up_weight, down_weight):
    normed = normalize(images, norm_gain)
    raw = jnp.einsum('itd,de->iet', normed.astype(jnp.float32), slot_map.astype(jnp.float32))
    dispatch, combine = weights_from(raw, normed, slot_map, logit_scale[0])
    slot_in = jnp.einsum('iet,itd->eid', dispatch.astype(jnp.float32), normed.astype(jnp.float32)).astype(jnp.bfloat16)
    hidden = jax.nn.gelu(jnp.einsum('eid,efd->eif', slot_in.astype(jnp.float32), up_weight.astype(jnp.float32))).astype(jnp.bfloat16)
    slot_out = jnp.einsum('eif,efd->eid', hidden.astype(jnp.float32), down_weight.astype(jnp.float32)).astype(jnp.bfloat16)
    mixed = jnp.einsum('iet,eid->itd', combine.astype(jnp.float32), slot_out.astype(jnp.float32))
    return (images.astype(jnp.float32) + mixed).astype(jnp.bfloat16)
```

```python
import jax
import jax.numpy as jnp
from jax import lax
from jax.experimental import pallas as pl
from jax.experimental.pallas import tpu as pltpu
from jax.sharding import PartitionSpec as P

epsilon = 1e-06
LANES = 128
f32 = jnp.float32
bf16 = jnp.bfloat16
NT = (((1,), (1,)), ((), ()))
TN = (((0,), (0,)), ((), ()))


def packed_rows(width):
    return -(-(width // LANES) // 16) * 16


def to_pieces(values, flat_ref, piece_ref, copies):
    count, width = values.shape
    rows = piece_ref.shape[1]
    flat_ref[...] = jnp.zeros(flat_ref.shape, f32)
    for j in range(width // LANES):
        flat_ref[pl.ds(j, count, stride=rows), :] = values[:, j * LANES : (j + 1) * LANES]
    pieces = flat_ref[...].astype(bf16).reshape(count, rows, LANES)
    for c in range(copies):
        piece_ref[c * count : (c + 1) * count] = pieces


def from_pieces(piece_ref, flat_ref, width):
    count, rows, _ = piece_ref.shape
    flat_ref[...] = piece_ref[...].reshape(count * rows, LANES).astype(f32)
    parts = [flat_ref[pl.ds(j, count, stride=rows), :] for j in range(width // LANES)]
    return jnp.concatenate(parts, axis=1).astype(bf16)


def routing_kernel(scale_ref, images_ref, gain_ref, slots_ref, piece_ref, combine_ref, flat_ref, *, sections):
    values = images_ref[...].astype(f32)
    spread = jnp.mean(values * values, axis=-1, keepdims=True)
    normed = (values * lax.rsqrt(spread + epsilon) * gain_ref[...].astype(f32)).astype(bf16)
    slot_rows = slots_ref[...]
    raw = lax.dot_general(normed, slot_rows, NT, preferred_element_type=f32)
    wide = normed.astype(f32)
    token_norm = jnp.sqrt(jnp.sum(wide * wide, axis=-1, keepdims=True) + epsilon)
    columns = slot_rows.astype(f32)
    column_norm = jnp.sqrt(jnp.sum(columns * columns, axis=-1, keepdims=True) + epsilon)
    count = slot_rows.shape[0]
    column_row = jnp.transpose(jnp.broadcast_to(column_norm, (count, LANES)))[:1, :]
    scores = jnp.exp(scale_ref[0] * raw / (token_norm * column_row))
    dispatch = (scores / jnp.sum(scores, axis=0, keepdims=True)).astype(bf16)
    slot_in = lax.dot_general(dispatch, normed, TN, preferred_element_type=f32)
    to_pieces(slot_in, flat_ref, piece_ref, sections)
    combine = (scores / jnp.sum(scores, axis=1, keepdims=True)).astype(bf16)
    combine_ref[...] = jnp.concatenate([combine] * sections, axis=1)


def routing(scale, images, gain, slot_rows, sections):
    tokens, width = images.shape
    count = slot_rows.shape[0]
    rows = packed_rows(width)
    vmem = pl.BlockSpec(memory_space=pltpu.VMEM)
    return pl.pallas_call(
        lambda *refs: routing_kernel(*refs, sections=sections),
        out_shape=(
            jax.ShapeDtypeStruct((sections * count, rows, LANES), bf16),
            jax.ShapeDtypeStruct((tokens, sections * count), bf16),
        ),
        in_specs=[pl.BlockSpec(memory_space=pltpu.SMEM), vmem, vmem, vmem],
        out_specs=(vmem, vmem),
        scratch_shapes=[pltpu.VMEM((count * rows, LANES), f32)],
        name="routing",
    )(scale, images, gain, slot_rows)


def experts_kernel(piece_ref, up_hbm, down_hbm, out_ref, up_ref, down_ref, flat_ref, sems, *, chunk):
    hidden_rows, width = up_ref.shape
    steps = hidden_rows // chunk

    def copies(i):
        part = pl.ds(i * chunk, chunk)
        return (
            pltpu.make_async_copy(up_hbm.at[part], up_ref.at[part], sems.at[0, i]),
            pltpu.make_async_copy(down_hbm.at[part], down_ref.at[part], sems.at[1, i]),
        )

    for i in range(steps):
        for copy in copies(i):
            copy.start()
    inputs = from_pieces(piece_ref, flat_ref, width)
    total = None
    for i in range(steps):
        up_copy, down_copy = copies(i)
        up_copy.wait()
        part = slice(i * chunk, (i + 1) * chunk)
        hidden = lax.dot_general(inputs, up_ref[part, :], NT, preferred_element_type=f32)
        hidden = jax.nn.gelu(hidden).astype(bf16)
        down_copy.wait()
        term = jnp.dot(hidden, down_ref[part, :], preferred_element_type=f32)
        total = term if total is None else total + term
    to_pieces(total, flat_ref, out_ref, 1)


def experts(pieces, up, down):
    hidden_rows, width = up.shape
    count, rows, _ = pieces.shape
    chunk = next(c for c in (512, 256, 128, hidden_rows) if hidden_rows % c == 0)
    steps = hidden_rows // chunk
    vmem = pl.BlockSpec(memory_space=pltpu.VMEM)
    anywhere = pl.BlockSpec(memory_space=pl.ANY)
    return pl.pallas_call(
        lambda *refs: experts_kernel(*refs, chunk=chunk),
        out_shape=jax.ShapeDtypeStruct(pieces.shape, bf16),
        in_specs=[vmem, anywhere, anywhere],
        out_specs=vmem,
        scratch_shapes=[
            pltpu.VMEM((hidden_rows, width), bf16),
            pltpu.VMEM((hidden_rows, width), bf16),
            pltpu.VMEM((count * rows, LANES), f32),
            pltpu.SemaphoreType.DMA((2, steps)),
        ],
        name="experts",
    )(pieces, up, down)


def mixing_kernel(images_ref, combine_ref, piece_ref, out_ref, flat_ref):
    outputs = from_pieces(piece_ref, flat_ref, images_ref.shape[1])
    mixed = jnp.dot(combine_ref[...], outputs, preferred_element_type=f32)
    out_ref[...] = (images_ref[...].astype(f32) + mixed).astype(bf16)


def mixing(images, combine, pieces):
    count, rows, _ = pieces.shape
    vmem = pl.BlockSpec(memory_space=pltpu.VMEM)
    return pl.pallas_call(
        mixing_kernel,
        out_shape=jax.ShapeDtypeStruct(images.shape, bf16),
        in_specs=[vmem, vmem, vmem],
        out_specs=vmem,
        scratch_shapes=[pltpu.VMEM((count * rows, LANES), f32)],
        name="mixing",
    )(images, combine, pieces)


def exchange(pieces):
    return lax.all_to_all(pieces, ("section", "expert"), split_axis=0, concat_axis=0, tiled=True)


def solution(mesh):
    sections = mesh.shape["section"]

    def local(images, norm_gain, slot_map, logit_scale, up_weight, down_weight):
        own = images[0]
        pieces, combine = routing(logit_scale, own, norm_gain[None, :], slot_map.T, sections)
        arrived = exchange(pieces)
        results = experts(arrived, up_weight[0], down_weight[0])
        back = exchange(results)
        return mixing(own, combine, back)[None]

    return jax.shard_map(
        local,
        mesh=mesh,
        in_specs=(
            P(("section", "expert"), None, None),
            P(),
            P(),
            P(),
            P("expert", "section", None),
            P("expert", "section", None),
        ),
        out_specs=P(("section", "expert"), None, None),
        check_vma=False,
    )
```

```python
import jax
import jax.numpy as jnp
from jax import lax
from jax.experimental import pallas as pl
from jax.experimental.pallas import tpu as pltpu
from jax.sharding import PartitionSpec as P

epsilon = 1e-06
LANES = 128
SCOPED = 12 * 2**20
f32 = jnp.float32
bf16 = jnp.bfloat16
NT = (((1,), (1,)), ((), ()))
TN = (((0,), (0,)), ((), ()))


def packed_rows(width):
    return -(-(width // LANES) // 16) * 16


def to_pieces(values, flat_ref, piece_ref, copies):
    count, width = values.shape
    rows = piece_ref.shape[1]
    flat_ref[...] = jnp.zeros(flat_ref.shape, f32)
    for j in range(width // LANES):
        flat_ref[pl.ds(j, count, stride=rows), :] = values[:, j * LANES : (j + 1) * LANES]
    pieces = flat_ref[...].astype(bf16).reshape(count, rows, LANES)
    for c in range(copies):
        piece_ref[c * count : (c + 1) * count] = pieces


def from_pieces(piece_ref, flat_ref, width):
    count, rows, _ = piece_ref.shape
    flat_ref[...] = piece_ref[...].reshape(count * rows, LANES).astype(f32)
    parts = [flat_ref[pl.ds(j, count, stride=rows), :] for j in range(width // LANES)]
    return jnp.concatenate(parts, axis=1).astype(bf16)


def gain_row(gain_ref):
    parts = [gain_ref[pl.ds(j, LANES)].astype(f32).reshape(1, LANES) for j in range(0, gain_ref.shape[0], LANES)]
    return jnp.concatenate(parts, axis=1)


def routing_kernel(
    scale_ref, images_hbm, gain_hbm, slots_hbm, piece_ref, combine_ref, *refs, sections, parts
):
    images_ref, gain_ref, slots_ref, normed_ref, flat_ref, sems = refs
    tokens = images_ref.shape[0]
    chunk = tokens // parts
    blocks = [pl.ds(i * chunk, chunk) for i in range(parts)]
    small = [
        pltpu.make_async_copy(gain_hbm, gain_ref, sems.at[0]),
        pltpu.make_async_copy(slots_hbm, slots_ref, sems.at[1]),
    ]
    loads = [
        pltpu.make_async_copy(images_hbm.at[block], images_ref.at[block], sems.at[2 + i])
        for i, block in enumerate(blocks)
    ]
    for copy in small + loads:
        copy.start()
    for copy in small:
        copy.wait()
    gain = gain_row(gain_ref)
    slot_rows = slots_ref[...]
    columns = slot_rows.astype(f32)
    column_norm = jnp.sqrt(jnp.sum(columns * columns, axis=-1, keepdims=True) + epsilon)
    column_row = jnp.transpose(jnp.broadcast_to(column_norm, (slot_rows.shape[0], LANES)))[:1, :]
    scores = []
    for block, load in zip(blocks, loads):
        load.wait()
        values = images_ref[block, :].astype(f32)
        spread = jnp.mean(values * values, axis=-1, keepdims=True)
        normed = (values * lax.rsqrt(spread + epsilon) * gain).astype(bf16)
        normed_ref[block, :] = normed
        raw = lax.dot_general(normed, slot_rows, NT, preferred_element_type=f32)
        wide = normed.astype(f32)
        token_norm = jnp.sqrt(jnp.sum(wide * wide, axis=-1, keepdims=True) + epsilon)
        scores.append(jnp.exp(scale_ref[0] * raw / (token_norm * column_row)))
    scores = jnp.concatenate(scores, axis=0)
    dispatch = (scores / jnp.sum(scores, axis=0, keepdims=True)).astype(bf16)
    slot_in = lax.dot_general(dispatch, normed_ref[...], TN, preferred_element_type=f32)
    to_pieces(slot_in, flat_ref, piece_ref, sections)
    combine = (scores / jnp.sum(scores, axis=1, keepdims=True)).astype(bf16)
    combine_ref[...] = jnp.concatenate([combine] * sections, axis=1)


def in_hbm(array):
    return pltpu.with_memory_space_constraint(array, pltpu.MemorySpace.HBM)


def in_vmem(array):
    return pltpu.with_memory_space_constraint(array, pltpu.MemorySpace.VMEM)


def routing(scale, images, gain, slot_rows, sections):
    tokens, width = images.shape
    count = slot_rows.shape[0]
    rows = packed_rows(width)
    parts = 4 if tokens % 64 == 0 else 1
    vmem = pl.BlockSpec(memory_space=pltpu.VMEM)
    hbm = pl.BlockSpec(memory_space=pltpu.MemorySpace.HBM)
    return pl.pallas_call(
        lambda *refs: routing_kernel(*refs, sections=sections, parts=parts),
        out_shape=(
            pltpu.VMEM((sections * count, rows, LANES), bf16),
            pltpu.VMEM((tokens, sections * count), bf16),
        ),
        in_specs=[pl.BlockSpec(memory_space=pltpu.SMEM)] + [hbm] * 3,
        out_specs=(vmem, vmem),
        scratch_shapes=[
            pltpu.VMEM(images.shape, bf16),
            pltpu.VMEM(gain.shape, bf16),
            pltpu.VMEM(slot_rows.shape, bf16),
            pltpu.VMEM(images.shape, bf16),
            pltpu.VMEM((count * rows, LANES), f32),
            pltpu.SemaphoreType.DMA((2 + parts,)),
        ],
        compiler_params=pltpu.CompilerParams(vmem_limit_bytes=SCOPED),
        cost_estimate=pl.CostEstimate(flops=10**10, bytes_accessed=10**8, transcendentals=0),
        name="routing",
    )(scale, in_hbm(images), in_hbm(gain), in_hbm(slot_rows))


def experts_kernel(piece_ref, up_ref, down_ref, out_ref, flat_ref, *, chunk):
    hidden_rows, width = up_ref.shape
    inputs = from_pieces(piece_ref, flat_ref, width)
    total = None
    for i in range(0, hidden_rows, chunk):
        block = pl.ds(i, chunk)
        hidden = lax.dot_general(inputs, up_ref[block, :], NT, preferred_element_type=f32)
        hidden = jax.nn.gelu(hidden).astype(bf16)
        term = jnp.dot(hidden, down_ref[block, :], preferred_element_type=f32)
        total = term if total is None else total + term
    to_pieces(total, flat_ref, out_ref, 1)


def experts(pieces, up, down, chunk):
    count, rows, _ = pieces.shape
    vmem = pl.BlockSpec(memory_space=pltpu.VMEM)
    return pl.pallas_call(
        lambda *refs: experts_kernel(*refs, chunk=chunk),
        out_shape=pltpu.VMEM(pieces.shape, bf16),
        in_specs=[vmem, vmem, vmem],
        out_specs=vmem,
        scratch_shapes=[pltpu.VMEM((count * rows, LANES), f32)],
        compiler_params=pltpu.CompilerParams(vmem_limit_bytes=SCOPED),
        name="experts",
    )(in_vmem(pieces), in_vmem(up), in_vmem(down))


def mixing_kernel(images_ref, combine_ref, piece_ref, out_hbm, flat_ref, out_ref, sems, *, chunk):
    tokens, width = images_ref.shape
    outputs = from_pieces(piece_ref, flat_ref, width)
    copies = []
    for i in range(tokens // chunk):
        part = pl.ds(i * chunk, chunk)
        mixed = jnp.dot(combine_ref[part, :], outputs, preferred_element_type=f32)
        out_ref[part, :] = (images_ref[part, :].astype(f32) + mixed).astype(bf16)
        copies.append(pltpu.make_async_copy(out_ref.at[part], out_hbm.at[part], sems.at[i]))
        copies[-1].start()
    for copy in copies:
        copy.wait()


def mixing(images, combine, pieces):
    count, rows, _ = pieces.shape
    tokens, width = images.shape
    chunk = tokens // 4 if tokens % 64 == 0 else tokens
    vmem = pl.BlockSpec(memory_space=pltpu.VMEM)
    return pl.pallas_call(
        lambda *refs: mixing_kernel(*refs, chunk=chunk),
        out_shape=jax.ShapeDtypeStruct(images.shape, bf16),
        in_specs=[vmem, vmem, vmem],
        out_specs=pl.BlockSpec(memory_space=pl.ANY),
        scratch_shapes=[
            pltpu.VMEM((count * rows, LANES), f32),
            pltpu.VMEM((tokens, width), bf16),
            pltpu.SemaphoreType.DMA((tokens // chunk,)),
        ],
        compiler_params=pltpu.CompilerParams(vmem_limit_bytes=SCOPED),
        name="mixing",
    )(in_vmem(images), in_vmem(combine), in_vmem(pieces))


def exchange(pieces):
    return lax.all_to_all(pieces, ("section", "expert"), split_axis=0, concat_axis=0, tiled=True)


def solution(mesh):
    sections = mesh.shape["section"]

    def local(images, norm_gain, slot_map, logit_scale, up_weight, down_weight):
        own, up, down = images[0], up_weight[0], down_weight[0]
        hidden_rows = up.shape[0]
        chunk = next(c for c in (512, 256, 128, hidden_rows) if hidden_rows % c == 0)
        pieces, combine = routing(logit_scale, own, norm_gain, slot_map.T, sections)
        arrived = exchange(pieces)
        results = experts(arrived, up, down, chunk)
        back = exchange(results)
        return mixing(own, combine, back)[None]

    return jax.shard_map(
        local,
        mesh=mesh,
        in_specs=(
            P(("section", "expert"), None, None),
            P(),
            P(),
            P(),
            P("expert", "section", None),
            P("expert", "section", None),
        ),
        out_specs=P(("section", "expert"), None, None),
        check_vma=False,
    )
```

```python
import jax
import jax.numpy as jnp
from jax import lax
from jax.experimental import pallas as pl
from jax.experimental.pallas import tpu as pltpu
from jax.sharding import PartitionSpec as P

epsilon = 1e-06
LANES = 128
SUB = 4
SCOPED = 12 * 2**20
f32 = jnp.float32
bf16 = jnp.bfloat16
NT = (((1,), (1,)), ((), ()))
TN = (((0,), (0,)), ((), ()))


def packed_rows(width):
    return -(-(width // LANES) // SUB) * SUB


def to_pieces(values, flat_ref, piece_ref, copies):
    count, width = values.shape
    rows = packed_rows(width)
    flat_ref[...] = jnp.zeros(flat_ref.shape, f32)
    for j in range(width // LANES):
        flat_ref[pl.ds(j, count, stride=rows), :] = values[:, j * LANES : (j + 1) * LANES]
    groups = count * rows // SUB
    pieces = flat_ref[...].reshape(groups, SUB, LANES).astype(bf16)
    for c in range(copies):
        piece_ref[c * groups : (c + 1) * groups] = pieces


def from_pieces(piece_ref, flat_ref, width):
    rows = packed_rows(width)
    count = piece_ref.shape[0] * SUB // rows
    flat_ref[...] = piece_ref[...].astype(f32).reshape(count * rows, LANES)
    parts = [flat_ref[pl.ds(j, count, stride=rows), :] for j in range(width // LANES)]
    return jnp.concatenate(parts, axis=1).astype(bf16)


def gain_row(gain_ref):
    parts = [gain_ref[pl.ds(j, LANES)].astype(f32).reshape(1, LANES) for j in range(0, gain_ref.shape[0], LANES)]
    return jnp.concatenate(parts, axis=1)


def routing_kernel(
    scale_ref, images_hbm, gain_hbm, slots_hbm, piece_ref, combine_ref, *refs, sections, parts
):
    images_ref, gain_ref, slots_ref, normed_ref, flat_ref, sems = refs
    tokens = images_ref.shape[0]
    chunk = tokens // parts
    blocks = [pl.ds(i * chunk, chunk) for i in range(parts)]
    small = [
        pltpu.make_async_copy(gain_hbm, gain_ref, sems.at[0]),
        pltpu.make_async_copy(slots_hbm, slots_ref, sems.at[1]),
    ]
    loads = [
        pltpu.make_async_copy(images_hbm.at[block], images_ref.at[block], sems.at[2 + i])
        for i, block in enumerate(blocks)
    ]
    for copy in small + loads:
        copy.start()
    for copy in small:
        copy.wait()
    gain = gain_row(gain_ref)
    slot_rows = slots_ref[...]
    columns = slot_rows.astype(f32)
    column_norm = jnp.sqrt(jnp.sum(columns * columns, axis=-1, keepdims=True) + epsilon)
    column_row = jnp.transpose(jnp.broadcast_to(column_norm, (slot_rows.shape[0], LANES)))[:1, :]
    scores = []
    for block, load in zip(blocks, loads):
        load.wait()
        values = images_ref[block, :].astype(f32)
        spread = jnp.mean(values * values, axis=-1, keepdims=True)
        normed = (values * lax.rsqrt(spread + epsilon) * gain).astype(bf16)
        normed_ref[block, :] = normed
        raw = lax.dot_general(normed, slot_rows, NT, preferred_element_type=f32)
        wide = normed.astype(f32)
        token_norm = jnp.sqrt(jnp.sum(wide * wide, axis=-1, keepdims=True) + epsilon)
        scores.append(jnp.exp(scale_ref[0] * raw / (token_norm * column_row)))
    scores = jnp.concatenate(scores, axis=0)
    dispatch = (scores / jnp.sum(scores, axis=0, keepdims=True)).astype(bf16)
    slot_in = lax.dot_general(dispatch, normed_ref[...], TN, preferred_element_type=f32)
    to_pieces(slot_in, flat_ref, piece_ref, sections)
    combine = (scores / jnp.sum(scores, axis=1, keepdims=True)).astype(bf16)
    combine_ref[...] = jnp.concatenate([combine] * sections, axis=1)


def in_hbm(array):
    return pltpu.with_memory_space_constraint(array, pltpu.MemorySpace.HBM)


def in_vmem(array):
    return pltpu.with_memory_space_constraint(array, pltpu.MemorySpace.VMEM)


def routing(scale, images, gain, slot_rows, sections):
    tokens, width = images.shape
    count = slot_rows.shape[0]
    rows = packed_rows(width)
    parts = 2 if tokens % 32 == 0 else 1
    vmem = pl.BlockSpec(memory_space=pltpu.VMEM)
    hbm = pl.BlockSpec(memory_space=pltpu.MemorySpace.HBM)
    return pl.pallas_call(
        lambda *refs: routing_kernel(*refs, sections=sections, parts=parts),
        out_shape=(
            pltpu.VMEM((sections * count * rows // SUB, SUB, LANES), bf16),
            pltpu.VMEM((tokens, sections * count), bf16),
        ),
        in_specs=[pl.BlockSpec(memory_space=pltpu.SMEM)] + [hbm] * 3,
        out_specs=(vmem, vmem),
        scratch_shapes=[
            pltpu.VMEM(images.shape, bf16),
            pltpu.VMEM(gain.shape, bf16),
            pltpu.VMEM(slot_rows.shape, bf16),
            pltpu.VMEM(images.shape, bf16),
            pltpu.VMEM((count * rows, LANES), f32),
            pltpu.SemaphoreType.DMA((2 + parts,)),
        ],
        compiler_params=pltpu.CompilerParams(vmem_limit_bytes=SCOPED),
        cost_estimate=pl.CostEstimate(flops=10**10, bytes_accessed=10**8, transcendentals=0),
        name="routing",
    )(scale, in_hbm(images), in_hbm(gain), in_hbm(slot_rows))


def experts_kernel(piece_ref, up_ref, down_ref, out_ref, flat_ref, *, chunk):
    hidden_rows, width = up_ref.shape
    inputs = from_pieces(piece_ref, flat_ref, width)
    total = None
    for i in range(0, hidden_rows, chunk):
        block = pl.ds(i, chunk)
        hidden = lax.dot_general(inputs, up_ref[block, :], NT, preferred_element_type=f32)
        hidden = jax.nn.gelu(hidden).astype(bf16)
        term = jnp.dot(hidden, down_ref[block, :], preferred_element_type=f32)
        total = term if total is None else total + term
    to_pieces(total, flat_ref, out_ref, 1)


def experts(pieces, up, down, chunk):
    count = pieces.shape[0]
    rows = SUB
    vmem = pl.BlockSpec(memory_space=pltpu.VMEM)
    return pl.pallas_call(
        lambda *refs: experts_kernel(*refs, chunk=chunk),
        out_shape=pltpu.VMEM(pieces.shape, bf16),
        in_specs=[vmem, vmem, vmem],
        out_specs=vmem,
        scratch_shapes=[pltpu.VMEM((count * rows, LANES), f32)],
        compiler_params=pltpu.CompilerParams(vmem_limit_bytes=SCOPED),
        name="experts",
    )(in_vmem(pieces), in_vmem(up), in_vmem(down))


def mixing_kernel(images_ref, combine_ref, piece_ref, out_hbm, flat_ref, out_ref, sems, *, chunk):
    tokens, width = images_ref.shape
    outputs = from_pieces(piece_ref, flat_ref, width)
    copies = []
    for i in range(tokens // chunk):
        part = pl.ds(i * chunk, chunk)
        mixed = jnp.dot(combine_ref[part, :], outputs, preferred_element_type=f32)
        out_ref[part, :] = (images_ref[part, :].astype(f32) + mixed).astype(bf16)
        copies.append(pltpu.make_async_copy(out_ref.at[part], out_hbm.at[part], sems.at[i]))
        copies[-1].start()
    for copy in copies:
        copy.wait()


def mixing(images, combine, pieces):
    count = pieces.shape[0]
    rows = SUB
    tokens, width = images.shape
    chunk = tokens // 4 if tokens % 64 == 0 else tokens
    vmem = pl.BlockSpec(memory_space=pltpu.VMEM)
    return pl.pallas_call(
        lambda *refs: mixing_kernel(*refs, chunk=chunk),
        out_shape=jax.ShapeDtypeStruct(images.shape, bf16),
        in_specs=[vmem, vmem, vmem],
        out_specs=pl.BlockSpec(memory_space=pl.ANY),
        scratch_shapes=[
            pltpu.VMEM((count * rows, LANES), f32),
            pltpu.VMEM((tokens, width), bf16),
            pltpu.SemaphoreType.DMA((tokens // chunk,)),
        ],
        compiler_params=pltpu.CompilerParams(vmem_limit_bytes=SCOPED),
        name="mixing",
    )(in_vmem(images), in_vmem(combine), in_vmem(pieces))


def exchange(pieces):
    return lax.all_to_all(pieces, ("section", "expert"), split_axis=0, concat_axis=0, tiled=True)


def solution(mesh):
    sections = mesh.shape["section"]

    def local(images, norm_gain, slot_map, logit_scale, up_weight, down_weight):
        own, up, down = images[0], up_weight[0], down_weight[0]
        hidden_rows = up.shape[0]
        chunk = next(c for c in (1280, 640, hidden_rows) if hidden_rows % c == 0)
        pieces, combine = routing(logit_scale, own, norm_gain, slot_map.T, sections)
        arrived = exchange(pieces)
        results = experts(arrived, up, down, chunk)
        back = exchange(results)
        return mixing(own, combine, back)[None]

    return jax.shard_map(
        local,
        mesh=mesh,
        in_specs=(
            P(("section", "expert"), None, None),
            P(),
            P(),
            P(),
            P("expert", "section", None),
            P("expert", "section", None),
        ),
        out_specs=P(("section", "expert"), None, None),
        check_vma=False,
    )
```
